32 devices in a mesh: replica: 16 (over z, y, core), shard: 2 (over x).
Axes of the slice: x: 2, y: 2, z: 4, core: 2. Of those that a mesh axis runs over, the one named last changes fastest.
Arguments:
- weight: bfloat16 [256, 8192], P(None, 'shard'), may hold values from -6 to 6
- momentum: float32 [16, 256, 8192], P('replica', None, 'shard'), may hold values from -6 to 6
- grad: bfloat16 [16, 256, 8192], P('replica', None, 'shard'), may hold values from -6 to 6
- positions: int32 [16, 4, 128, 32], P('replica', None, 'shard'), may hold values from 0 to 4095, as said below
Outputs:
- kept_state: float32 [16, 256, 8192], P('replica', None, 'shard')
- direction: bfloat16 [256, 8192], P(None, 'shard')
- new_weight: bfloat16 [256, 8192], replicated
The draws below stay inside these ranges and needn't reach their ends.
Inputs may be any that keep to these rules, and one draw needn't show every extreme that they name: The 32 positions of one block on one replica are distinct; replicas choose independently.
All inputs are finite; a program needn't handle non-finite values.
Results may differ from the reference program's by a relative error of at most 0.001.
Values may be sent and summed in bfloat16 or wider, within the bound.
A program may use at most 128 MiB of HBM per device.

```python
import math
import jax
import jax.numpy as jnp
from jax import lax

D = 8192
GROUP = 64
TOPK = 32
ROWS = 256
REPLICAS = 16


def draw_positions(key, part):
    shape = (REPLICAS, ROWS // GROUP, D // GROUP, GROUP * GROUP)
    scores = jax.random.randint(key, shape, 0, 1 << 18, dtype=jnp.int32) * (GROUP * GROUP)
    scores = scores + jnp.arange(GROUP * GROUP, dtype=jnp.int32)
    chosen = lax.top_k(scores, TOPK)[1]
    return chosen.astype(jnp.int32)


def block_levels(key, extent, split, smallest, top_value):
    level, own = 1.0, jax.random.fold_in(key, 6)
    for axis_at, shards_of in split:
        heights = jnp.exp(jax.random.uniform(jax.random.fold_in(own, axis_at), (shards_of,), jnp.float32, smallest / len(split), top_value / len(split)))
        level = level * jnp.repeat(heights, extent[axis_at] // shards_of).reshape([-1 if axis == axis_at else 1 for axis in range(len(extent))])
    return level


def centred(key, dims, width, bound, split=(), kind=jnp.bfloat16):
    values = jax.random.normal(key, dims, jnp.float32) * width
    if len(split) > 0:
        values = block_levels(key, dims, split, -0.22, 0.18) * values
    return jnp.clip(values, min=-bound, max=bound).astype(kind)


def setup_inputs(seed: int = 0) -> dict:
    splits = jax.random.split(jax.random.key(seed), 5)
    return {
        "weight": centred(splits[0], (ROWS, D), 1.0, 6.0, ((1, 2),)),
        "momentum": centred(splits[1], (REPLICAS, ROWS, D), 1.0, 6.0, ((0, 16), (2, 2)), jnp.float32),
        "grad": centred(splits[2], (REPLICAS, ROWS, D), 1.0, 6.0, ((0, 16), (2, 2))),
        "positions": draw_positions(jax.random.fold_in(splits[4], 71), 0),
    }


beta_decay = 0.9
step_rate = 0.02

def dct_basis():
    freq = jnp.arange(GROUP, dtype=jnp.float32)[:, None]
    cells = jnp.arange(GROUP, dtype=jnp.float32)[None, :]
    scales = jnp.where(freq == 0, math.sqrt(1.0 / GROUP), math.sqrt(2.0 / GROUP))
    return scales * jnp.cos(math.pi * (2.0 * cells + 1.0) * freq / (2.0 * GROUP))

def reference(weight, momentum, grad, positions):
    basis_table = dct_basis()
    row_blocks = ROWS // GROUP
    col_blocks = D // GROUP
    row_index = jnp.arange(row_blocks, dtype=jnp.int32)[:, None, None]
    col_index = jnp.arange(col_blocks, dtype=jnp.int32)[None, :, None]

    def scatter_coeffs(values, where):
        flat = jnp.zeros((row_blocks, col_blocks, GROUP * GROUP), jnp.float32)
        flat = flat.at[row_index, col_index, where].add(values)
        return flat.reshape(row_blocks, col_blocks, GROUP, GROUP)

    def inverse(coeff_blocks):
        dense = jnp.einsum('ai,xyab,bj->xiyj', basis_table, coeff_blocks, basis_table, precision=lax.Precision.HIGHEST)
        return dense.reshape(ROWS, D)

    def one_replica(triple):
        state, slope, where = triple
        moved = beta_decay * state + slope.astype(jnp.float32)
        blocks = moved.reshape(row_blocks, GROUP, col_blocks, GROUP)
        coeff = jnp.einsum('ai,xiyj,bj->xyab', basis_table, blocks, basis_table, precision=lax.Precision.HIGHEST)
        coeff = coeff.reshape(row_blocks, col_blocks, GROUP * GROUP)
        picked = jnp.take_along_axis(coeff, where, axis=2)
        return (moved - inverse(scatter_coeffs(picked, where)), picked)
    kept_state, picked_all = lax.map(one_replica, (momentum, grad, positions))
    values = jnp.moveaxis(picked_all, 0, 2).reshape(row_blocks, col_blocks, REPLICAS * TOPK)
    where = jnp.moveaxis(positions, 0, 2).reshape(row_blocks, col_blocks, REPLICAS * TOPK)
    smooth = jnp.tanh(inverse(scatter_coeffs(values, where)))
    direction = smooth.astype(jnp.bfloat16)
    new_weight = (weight.astype(jnp.float32) - step_rate * smooth).astype(jnp.bfloat16)
    return (kept_state, direction, new_weight)
```

```python
import functools
import math

import jax
import jax.numpy as jnp
import numpy as np
from jax import lax
from jax.experimental import pallas as pl
from jax.experimental.pallas import tpu as pltpu
from jax.sharding import PartitionSpec as P

GROUP = 64
LANES = 128
WIDE = 256

beta_decay = 0.9
step_rate = 0.02

f32, bf16 = jnp.float32, jnp.bfloat16
MESH = pl.DeviceIdType.MESH


def basis_parts(blocks, transposed):
    k = np.arange(GROUP, dtype=np.float64)[:, None]
    i = np.arange(GROUP, dtype=np.float64)[None, :]
    scale = np.where(k == 0, math.sqrt(1.0 / GROUP), math.sqrt(2.0 / GROUP))
    c = scale * np.cos(math.pi * (2.0 * i + 1.0) * k / (2.0 * GROUP))
    if transposed:
        c = c.T
    full = np.kron(np.eye(blocks), c).astype(np.float32)
    high = full.astype(bf16)
    low = (full - high.astype(np.float32)).astype(bf16)
    return np.stack([high, low])


def split(x):
    high = x.astype(bf16)
    return high, (x - high.astype(f32)).astype(bf16)


def dot(a, b):
    return jnp.dot(a, b, preferred_element_type=f32)


def dot_t(a, b):
    return lax.dot_general(a, b, (((1,), (1,)), ((), ())), preferred_element_type=f32)


def left(m, x):
    high, low = split(x)
    return dot(m[0], high) + (dot(m[0], low) + dot(m[1], high))


def right(x, m):
    high, low = split(x)
    return dot(high, m[0]) + (dot(low, m[0]) + dot(high, m[1]))


def down(rows):
    return lax.broadcasted_iota(jnp.int32, (rows, LANES), 0).astype(f32)


def lane_offset(topk):
    lane = lax.broadcasted_iota(jnp.int32, (1, LANES), 1)
    return (lane // topk * GROUP).astype(f32)


def place(pos, topk):
    a = jnp.floor(pos * (1.0 / GROUP))
    return a, pos - a * GROUP + lane_offset(topk)


def own_kernel(nx, topk, mom, grad, pos, lf, rt, li, ri, kept, sent):
    moved = beta_decay * mom[0] + grad[0].astype(f32)
    coeff = right(left(lf, moved), rt)
    spots = pos[0]
    a, b = place(spots, topk)
    rows, cols = down(GROUP), down(WIDE)
    picked, own = [], []
    for x in range(nx):
        part = coeff[x * GROUP : (x + 1) * GROUP]
        at_row = rows == a[x : x + 1]
        hot_a = jnp.where(at_row, 1.0, 0.0).astype(bf16)
        hot_b = jnp.where(cols == b[x : x + 1], 1.0, 0.0).astype(bf16)
        own.append(part * dot_t(hot_a, hot_b))
        high, low = split(part)
        found = dot(jnp.concatenate([high, low], axis=0), hot_b)
        found = found[:GROUP] + found[GROUP:]
        picked.append(jnp.sum(jnp.where(at_row, found, 0.0), axis=0, keepdims=True))
    kept[0] = moved - right(left(li, jnp.concatenate(own, axis=0)), ri)
    sent[0] = jnp.concatenate(picked + [spots], axis=0)


def own_part(mom, grad, pos, topk, interpret=False):
    _, rows, width = mom.shape
    nx = rows // GROUP
    steps = width // WIDE
    blocks = WIDE // GROUP
    whole = lambda n: pl.BlockSpec((2, n, n), lambda g: (0, 0, 0))
    return pl.pallas_call(
        functools.partial(own_kernel, nx, topk),
        grid=(steps,),
        in_specs=[
            pl.BlockSpec((1, rows, WIDE), lambda g: (0, 0, g)),
            pl.BlockSpec((1, rows, WIDE), lambda g: (0, 0, g)),
            pl.BlockSpec((1, nx, LANES), lambda g: (g, 0, 0)),
            whole(rows), whole(WIDE), whole(rows), whole(WIDE),
        ],
        out_specs=[
            pl.BlockSpec((1, rows, WIDE), lambda g: (0, 0, g)),
            pl.BlockSpec((1, 2 * nx, LANES), lambda g: (g, 0, 0)),
        ],
        out_shape=[
            jax.ShapeDtypeStruct((1, rows, width), f32),
            jax.ShapeDtypeStruct((steps, 2 * nx, LANES), f32),
        ],
        interpret=interpret,
        name="own_part",
    )(
        mom, grad, pos,
        basis_parts(nx, False), basis_parts(blocks, True),
        basis_parts(nx, True), basis_parts(blocks, False),
    )


def swap_kernel(reps, shards, mine, got, send_sem, recv_sem, own_sem):
    r, s = lax.axis_index("replica"), lax.axis_index("shard")
    me = r * shards + s
    total = reps * shards
    keep = pltpu.make_async_copy(mine.at[lax.rem(r, 2)], got.at[s, r], own_sem)
    keep.start()

    def push(step):
        to = lax.rem(me + step, total)
        to_r, to_s = to // shards, lax.rem(to, shards)
        return pltpu.make_async_remote_copy(
            src_ref=mine.at[lax.rem(to_r, 2)],
            dst_ref=got.at[s, r],
            send_sem=send_sem.at[step],
            recv_sem=recv_sem.at[step],
            device_id=(to_r, to_s),
            device_id_type=MESH,
        )

    def come(step):
        of = lax.rem(me - step + total, total)
        of_r, of_s = of // shards, lax.rem(of, shards)
        return pltpu.make_async_remote_copy(
            src_ref=mine.at[0],
            dst_ref=got.at[of_s, of_r],
            send_sem=send_sem.at[step],
            recv_sem=recv_sem.at[step],
            device_id=(of_r, of_s),
            device_id_type=MESH,
        )

    @pl.loop(1, total)
    def _(step):
        push(step).start()

    @pl.loop(1, total)
    def _(step):
        push(step).wait_send()
        come(step).wait_recv()

    keep.wait()


def swap(mine, reps, shards):
    return pl.pallas_call(
        functools.partial(swap_kernel, reps, shards),
        in_specs=[pl.BlockSpec(memory_space=pltpu.VMEM)],
        out_specs=pl.BlockSpec(memory_space=pltpu.VMEM),
        out_shape=jax.ShapeDtypeStruct((shards, reps) + mine.shape[1:], f32),
        scratch_shapes=[
            pltpu.SemaphoreType.DMA((reps * shards,)),
            pltpu.SemaphoreType.DMA((reps * shards,)),
            pltpu.SemaphoreType.DMA,
        ],
        compiler_params=pltpu.CompilerParams(has_side_effects=True),
        name="swap",
    )(mine)


def sum_kernel(nx, topk, reps, _, data, weight, li, ri, smooth_out, weight_out):
    rows, cols = down(GROUP), down(WIDE)
    tiles = []
    for x in range(nx):
        lefts, rights = [], []
        for r in range(reps):
            tile = data[0, r, 0]
            a, b = place(tile[nx + x : nx + x + 1], topk)
            high, low = split(tile[x : x + 1])
            at_row = rows == a
            lefts.append(jnp.concatenate([
                jnp.where(at_row, high.astype(f32), 0.0).astype(bf16),
                jnp.where(at_row, low.astype(f32), 0.0).astype(bf16),
            ], axis=0))
            rights.append(jnp.where(cols == b, 1.0, 0.0).astype(bf16))
        both = dot_t(jnp.concatenate(lefts, axis=1), jnp.concatenate(rights, axis=1))
        tiles.append(both[:GROUP] + both[GROUP:])
    smooth = jnp.tanh(right(left(li, jnp.concatenate(tiles, axis=0)), ri))
    smooth_out[...] = smooth.astype(bf16)
    weight_out[...] = (weight[...].astype(f32) - step_rate * smooth).astype(bf16)


def sum_part(shard, data, weight, topk, interpret=False):
    rows, width = weight.shape
    nx = rows // GROUP
    reps = data.shape[1]
    blocks = WIDE // GROUP
    column = pl.BlockSpec((rows, WIDE), lambda g, s: (0, g))
    whole = lambda n: pl.BlockSpec((2, n, n), lambda g, s: (0, 0, 0))
    return pl.pallas_call(
        functools.partial(sum_kernel, nx, topk, reps),
        grid_spec=pltpu.PrefetchScalarGridSpec(
            num_scalar_prefetch=1,
            grid=(width // WIDE,),
            in_specs=[
                pl.BlockSpec((1, reps, 1, 2 * nx, LANES), lambda g, s: (s[0], 0, g, 0, 0)),
                column, whole(rows), whole(WIDE),
            ],
            out_specs=[column, column],
        ),
        out_shape=[jax.ShapeDtypeStruct((rows, width), bf16)] * 2,
        interpret=interpret,
        name="sum_part",
    )(shard, data, weight, basis_parts(nx, True), basis_parts(blocks, False))


def per_device(reps, shards, weight, momentum, grad, positions):
    rows, width = weight.shape
    _, nx, ny, topk = positions.shape
    half = width // 2
    steps = width // WIDE
    r, s = lax.axis_index("replica"), lax.axis_index("shard")
    core = lax.rem(r, 2)

    mine_w = lax.dynamic_slice(weight, (0, core * half), (rows, half))
    weights = [mine_w] + [
        lax.ppermute(mine_w, "shard", [(i, (i + d) % shards) for i in range(shards)])
        for d in range(1, shards)
    ]

    pos = positions[0].astype(f32).reshape(nx, steps, LANES).transpose(1, 0, 2)
    kept, sent = own_part(momentum, grad, pos, topk)
    got = swap(sent.reshape(2, steps // 2, 2 * nx, LANES), reps, shards)

    pairs = [(i, i ^ 1) for i in range(reps)]
    flip = lambda x: lax.ppermute(x, "replica", pairs)
    order = lambda a, b: [jnp.where(core == 0, a, b), jnp.where(core == 0, b, a)]
    pieces, direction = [], None
    for d in range(shards):
        of = lax.rem(s - d + shards, shards)
        smooth, updated = sum_part(of.reshape(1).astype(jnp.int32), got, weights[d], topk)
        if d == 0:
            direction = jnp.concatenate(order(smooth, flip(smooth)), axis=1)
        pieces.append((updated, flip(updated)))

    columns = []
    for t in range(shards):
        d = lax.rem(s - t + shards, shards)
        a, b = pieces[0]
        for e in range(1, shards):
            a = jnp.where(d == e, pieces[e][0], a)
            b = jnp.where(d == e, pieces[e][1], b)
        columns += order(a, b)
    return (kept, direction, jnp.concatenate(columns, axis=1))


def solution(mesh):
    reps, shards = mesh.shape["replica"], mesh.shape["shard"]
    in_specs = (
        P(None, "shard"),
        P("replica", None, "shard"),
        P("replica", None, "shard"),
        P("replica", None, "shard", None),
    )
    out_specs = (P("replica", None, "shard"), P(None, "shard"), P())
    return jax.shard_map(
        functools.partial(per_device, reps, shards),
        mesh=mesh, in_specs=in_specs, out_specs=out_specs, check_vma=False,
    )
```
